256 devices in a mesh: seq: 16 (over y, x), width: 16 (over z, core).
Axes of the slice: x: 4, y: 4, z: 8, core: 2. Of those that a mesh axis runs over, the one named last changes fastest.
Arguments:
- leak_rate: float32 [1, 32768, 2048], P(None, 'seq', 'width'), may hold values from 0.2 to 2
- signal_in: bfloat16 [1, 32768, 2048], P(None, 'seq', 'width'), may hold values from -6 to 6
- norm_gain: float32 [2048], P('width'), may hold values from 0.25 to 1.75
Outputs:
- mixed_out: bfloat16 [1, 32768, 2048], P(None, 'seq', 'width')
The draws below stay inside these ranges and needn't reach their ends.
All inputs are finite; a program needn't handle non-finite values.
Results may differ from the reference program's by a relative error of at most 0.001.
Values sent between devices are 32-bit elements; how exact they have to be, the bound alone decides.
No kernel may reach another device: no remote copies, remote signals or barrier semaphores. Data moves between devices by JAX's collectives and lax.ppermute only.
A program may use at most 64 MiB of HBM per device.

```python
import jax
import jax.numpy as jnp
from jax import lax

BATCH = 1
CHANNELS = 2048
LENGTH = 32768


def steps_of(own_key, dims, cuts, low, high):
    def one(position, blocks):
        heights = jax.random.uniform(jax.random.fold_in(jax.random.fold_in(own_key, 6), position), (blocks,), jnp.float32, low / len(cuts), high / len(cuts))
        return jnp.repeat(jnp.exp(heights), dims[position] // blocks).reshape((-1,) + (1,) * (len(dims) - position - 1))

    factor_of = one(*cuts[0])
    for cut in cuts[1:]:
        factor_of = factor_of * one(*cut)
    return factor_of


def bell_draw(rng, shape, scale, limit, shards=(), held_as=jnp.bfloat16):
    loudness = steps_of(rng, shape, shards, -0.22, 0.18) if shards else 1.0
    drawn = jax.random.normal(rng, shape, jnp.float32) * scale * loudness
    return jnp.minimum(jnp.maximum(drawn, -limit), limit).astype(held_as)


def setup_inputs(seed: int = 0) -> dict:
    seeds = jax.random.split(jax.random.key(seed), 4)
    leak_rate = jnp.clip(0.2 + 1.8 * jax.random.uniform(seeds[0], (BATCH, LENGTH, CHANNELS), jnp.float32) ** steps_of(seeds[0], (BATCH, LENGTH, CHANNELS), ((1, 16), (2, 16)), -0.2, 0.2), 0.2, 2.0)
    signal_in = bell_draw(seeds[1], (BATCH, LENGTH, CHANNELS), 1.0, 6.0, ((1, 16), (2, 16)))
    norm_gain = jnp.clip(1.0 + 0.15 * jax.random.normal(seeds[2], (CHANNELS,), jnp.float32), 0.25, 1.75)
    return {"leak_rate": leak_rate, "signal_in": signal_in, "norm_gain": norm_gain}


def join_pair(earlier, later):
    return (earlier[0] * later[0], later[0] * earlier[1] + later[1])

def reference(leak_rate, signal_in, norm_gain):
    keep = jnp.exp(-leak_rate / LENGTH)
    push = signal_in.astype(jnp.float32) * LENGTH ** (-0.5)
    forward = lax.associative_scan(join_pair, (keep, push), axis=1)[1]
    backward = lax.associative_scan(join_pair, (keep, push), axis=1, reverse=True)[1]
    states = forward + backward
    power = lax.optimization_barrier(jnp.mean(states * states, axis=-1, keepdims=True))
    mixed_out = (states * lax.rsqrt(power + 1e-06) * norm_gain).astype(jnp.bfloat16)
    return mixed_out
```

```python
import functools

import jax
import jax.numpy as jnp
from jax import lax
from jax.experimental import pallas as pl
from jax.experimental.pallas import tpu as pltpu
from jax.sharding import PartitionSpec as P

LANES = 128
SUB = 8
F32 = jnp.float32
VMEM = pl.BlockSpec(memory_space=pltpu.VMEM)
SMEM = pl.BlockSpec(memory_space=pltpu.SMEM)


def groups_of(rows):
    steps = rows // SUB
    short = steps // 4 - 4
    assert rows % SUB == 0 and short % 8 == 4 and short + 68 <= LANES
    cuts, at = [], 0
    for length in (short, short, short + 8, short + 8):
        cuts.append((at * SUB, at, length))
        at += length
    assert at == steps
    return cuts


def rows_at(group, step):
    first, _, length = group
    return pl.ds(first + step, SUB, stride=length)


def earlier_sublanes(x, by, fill):
    row = lax.broadcasted_iota(jnp.int32, x.shape, 0)
    return jnp.where(row >= by, pltpu.roll(x, by, 0), fill)


def later_sublanes(x, by, fill):
    row = lax.broadcasted_iota(jnp.int32, x.shape, 0)
    return jnp.where(row < SUB - by, pltpu.roll(x, SUB - by, 0), fill)


def scan_sublanes(product, total, shifted):
    for by in (1, 2, 4):
        total = total + product * shifted(total, by, 0.0)
        product = product * shifted(product, by, 1.0)
    return product, total


def all_steps(groups, body, state, reverse=False):
    shortest = min(length for _, _, length in groups)
    tail = range(shortest, max(length for _, _, length in groups))
    state = list(state)

    def tails(order):
        for step in order:
            for g, (_, _, length) in enumerate(groups):
                if step < length:
                    state[g] = body(g, step, state[g])

    if reverse:
        tails(reversed(tail))

    def one(i, carry):
        step = shortest - 1 - i if reverse else i
        return tuple(body(g, step, carry[g]) for g in range(len(groups)))

    state = list(lax.fori_loop(0, shortest, one, tuple(state), unroll=4))
    if not reverse:
        tails(tail)
    return state


def summary_kernel(total_length, leak_ref, signal_ref, ends_ref, parts_ref, keep_ref, push_ref, rows_ref):
    rows = leak_ref.shape[0]
    groups = groups_of(rows)
    scale = total_length ** (-0.5)

    def widen(i, _):
        at = pl.ds(pl.multiple_of(i * 16, 16), 16)
        rows_ref[at, :] = signal_ref[at, :].astype(F32) * scale
        return 0

    lax.fori_loop(0, rows // 16, widen, 0, unroll=8)

    def body(g, step, state):
        product, forward, backward = state
        keep = jnp.exp(-leak_ref[rows_at(groups[g], step), :] / total_length)
        push = rows_ref[rows_at(groups[g], step), :]
        keep_ref[groups[g][1] + step] = keep
        push_ref[groups[g][1] + step] = push
        return (product * keep, forward * keep + push, backward + product * push)

    zero = jnp.zeros((SUB, LANES), F32)
    state = all_steps(groups, body, [(zero + 1.0, zero, zero)] * len(groups))
    ends = []
    for g, (product, forward, backward) in enumerate(state):
        whole, forwards = scan_sublanes(product, forward, earlier_sublanes)
        turned, backwards = scan_sublanes(product, backward, later_sublanes)
        parts_ref[4 * g] = whole
        parts_ref[4 * g + 1] = forwards
        parts_ref[4 * g + 2] = turned
        parts_ref[4 * g + 3] = backwards
        ends.append((whole[SUB - 1 :], forwards[SUB - 1 :], backwards[:1]))
    product, forward, backward = ends[0][0], ends[0][1], ends[-1][2]
    for whole, forwards, _ in ends[1:]:
        product, forward = product * whole, forward * whole + forwards
    for whole, _, backwards in reversed(ends[:-1]):
        backward = backwards + whole * backward
    ends_ref[...] = jnp.concatenate([product, forward, backward, jnp.zeros_like(product)], axis=0)


def states_kernel(here_ref, all_ends_ref, parts_ref, keep_ref, push_ref, states_ref, squares_ref):
    groups = groups_of(keep_ref.shape[0] * SUB)
    here = here_ref[0]
    devices = all_ends_ref.shape[0]
    forward = jnp.zeros((1, LANES), F32)
    backward = jnp.zeros((1, LANES), F32)
    for d in range(devices):
        joined = forward * all_ends_ref[d, 0:1] + all_ends_ref[d, 1:2]
        forward = jnp.where(d < here, joined, forward)
        e = devices - 1 - d
        joined = backward * all_ends_ref[e, 0:1] + all_ends_ref[e, 2:3]
        backward = jnp.where(e > here, joined, backward)

    entering_forward, entering_backward = [], [None] * len(groups)
    for g in range(len(groups)):
        whole, forwards = parts_ref[4 * g], parts_ref[4 * g + 1]
        entering_forward.append(
            earlier_sublanes(forwards, 1, 0.0) + earlier_sublanes(whole, 1, 1.0) * forward
        )
        forward = forwards[SUB - 1 :] + whole[SUB - 1 :] * forward
    for g in reversed(range(len(groups))):
        whole, backwards = parts_ref[4 * g + 2], parts_ref[4 * g + 3]
        entering_backward[g] = (
            later_sublanes(backwards, 1, 0.0) + later_sublanes(whole, 1, 1.0) * backward
        )
        backward = backwards[:1] + whole[:1] * backward

    def forth(g, step, state):
        at = groups[g][1] + step
        state = state * keep_ref[at] + push_ref[at]
        states_ref[at] = state
        return state

    all_steps(groups, forth, entering_forward)
    lane = lax.broadcasted_iota(jnp.int32, (SUB, LANES), 1)
    short = groups[0][2]

    def back(g, step, state):
        state, sums = state
        at = groups[g][1] + step
        state = state * keep_ref[at] + push_ref[at]
        both = states_ref[at] + state
        states_ref[at] = both
        power = jnp.sum(both * both, axis=1, keepdims=True)
        sums = jnp.where(lane == step + (short if g >= 2 else 0), power, sums)
        return state, sums

    zero = jnp.zeros((SUB, LANES), F32)
    done = all_steps(groups, back, [(b, zero) for b in entering_backward], reverse=True)
    for half in (0, 1):
        squares_ref[pl.ds(half * SUB, SUB), :] = jnp.where(lane < short, done[half][1], done[half + 2][1])


def norm_kernel(channels, all_squares_ref, states_ref, gain_ref, out_ref, rows_ref):
    rows = out_ref.shape[0]
    groups = groups_of(rows)
    short = groups[0][2]
    power = jnp.sum(all_squares_ref[...], axis=0) / channels
    scale = lax.rsqrt(power + 1e-06)
    halves = (scale[:SUB], scale[SUB:])
    gain = jnp.broadcast_to(gain_ref[...], (SUB, LANES))
    for g, (_, first, length) in enumerate(groups):
        for step in range(length):
            lane = step + (short if g >= 2 else 0)
            factor = jnp.broadcast_to(halves[g % 2][:, lane : lane + 1], (SUB, LANES))
            rows_ref[rows_at(groups[g], step), :] = states_ref[first + step] * factor * gain

    def narrow(i, _):
        at = pl.ds(pl.multiple_of(i * 16, 16), 16)
        out_ref[at, :] = rows_ref[at, :].astype(out_ref.dtype)
        return 0

    lax.fori_loop(0, rows // 16, narrow, 0, unroll=8)


def params():
    return pltpu.CompilerParams(vmem_limit_bytes=12 * 1024 * 1024)


def copies(x, axis):
    x = jnp.broadcast_to(x[None], (lax.axis_size(axis), *x.shape))
    return lax.all_to_all(x, axis, 0, 0, tiled=True)


def per_device(leak_rate, signal_in, norm_gain):
    rows, channels = leak_rate.shape[1], leak_rate.shape[2]
    total_length = rows * lax.axis_size("seq")
    steps = rows // SUB
    blocks = jax.ShapeDtypeStruct((steps, SUB, LANES), F32)
    ends, parts, keep, push = pl.pallas_call(
        functools.partial(summary_kernel, total_length),
        out_shape=(
            jax.ShapeDtypeStruct((4, LANES), F32),
            jax.ShapeDtypeStruct((16, SUB, LANES), F32),
            blocks,
            blocks,
        ),
        in_specs=[VMEM] * 2,
        out_specs=(VMEM,) * 4,
        scratch_shapes=[pltpu.VMEM((rows, LANES), F32)],
        compiler_params=params(),
        name="summary",
    )(leak_rate[0], signal_in[0])
    all_ends = copies(ends, "seq")
    here = lax.axis_index("seq").astype(jnp.int32).reshape(1)
    states, squares = pl.pallas_call(
        states_kernel,
        out_shape=(blocks, jax.ShapeDtypeStruct((2 * SUB, LANES), F32)),
        in_specs=[SMEM] + [VMEM] * 4,
        out_specs=(VMEM,) * 2,
        compiler_params=params(),
        name="states",
    )(here, all_ends, parts, keep, push)
    all_squares = copies(squares, "width")
    mixed = pl.pallas_call(
        functools.partial(norm_kernel, channels * lax.axis_size("width")),
        out_shape=jax.ShapeDtypeStruct((rows, LANES), jnp.bfloat16),
        in_specs=[VMEM] * 3,
        out_specs=VMEM,
        scratch_shapes=[pltpu.VMEM((rows, LANES), F32)],
        compiler_params=params(),
        name="norm",
    )(all_squares, states, norm_gain.reshape(1, channels))
    return mixed[None]


def solution(mesh):
    return jax.shard_map(
        per_device,
        mesh=mesh,
        in_specs=(P(None, "seq", "width"), P(None, "seq", "width"), P("width")),
        out_specs=P(None, "seq", "width"),
        check_vma=False,
    )
```

```python
import functools

import jax
import jax.numpy as jnp
from jax import lax
from jax.experimental import pallas as pl
from jax.experimental.pallas import tpu as pltpu
from jax.sharding import PartitionSpec as P

LANES = 128
SUB = 8
F32 = jnp.float32
VMEM = pl.BlockSpec(memory_space=pltpu.VMEM)
SMEM = pl.BlockSpec(memory_space=pltpu.SMEM)
HBM = pl.BlockSpec(memory_space=pltpu.HBM)


def groups_of(rows):
    steps = rows // SUB
    short = steps // 4 - 4
    assert rows % SUB == 0 and short % 8 == 4 and short + 68 <= LANES
    cuts, at = [], 0
    for length in (short, short, short + 8, short + 8):
        cuts.append((at * SUB, at, length))
        at += length
    assert at == steps
    return cuts


def rows_at(group, step):
    first, _, length = group
    return pl.ds(first + step, SUB, stride=length)


def earlier_sublanes(x, by, fill):
    row = lax.broadcasted_iota(jnp.int32, x.shape, 0)
    return jnp.where(row >= by, pltpu.roll(x, by, 0), fill)


def later_sublanes(x, by, fill):
    row = lax.broadcasted_iota(jnp.int32, x.shape, 0)
    return jnp.where(row < SUB - by, pltpu.roll(x, SUB - by, 0), fill)


def scan_sublanes(product, total, shifted):
    for by in (1, 2, 4):
        total = total + product * shifted(total, by, 0.0)
        product = product * shifted(product, by, 1.0)
    return product, total


def all_steps(groups, body, state, reverse=False):
    state = dict(state)
    longest = max(groups[g][2] for g in state)
    for step in reversed(range(longest)) if reverse else range(longest):
        for g in state:
            if step < groups[g][2]:
                state[g] = body(g, step, state[g])
    return state


def rows_of(group):
    first, _, length = group
    return pl.ds(first, length * SUB)


def summary_kernel(
    total_length,
    here_ref,
    leak_hbm,
    signal_hbm,
    gain_hbm,
    ends_ref,
    parts_ref,
    keep_ref,
    push_ref,
    gain_ref,
    leak_ref,
    signal_ref,
    rows_ref,
    arrived,
    gain_arrived,
):
    groups = groups_of(leak_ref.shape[0])
    scale = total_length ** (-0.5)
    loads = []
    for g, group in enumerate(groups):
        at = rows_of(group)
        loads.append(
            (
                pltpu.make_async_copy(leak_hbm.at[at], leak_ref.at[at], arrived.at[0, g]),
                pltpu.make_async_copy(signal_hbm.at[at], signal_ref.at[at], arrived.at[1, g]),
            )
        )
        for load in loads[-1]:
            load.start()
    gain_load = pltpu.make_async_copy(gain_hbm, gain_ref, gain_arrived)
    gain_load.start()

    def body(g, step, state):
        product, forward, backward = state
        keep = jnp.exp(-leak_ref[rows_at(groups[g], step), :] / total_length)
        push = rows_ref[rows_at(groups[g], step), :]
        keep_ref[groups[g][1] + step] = keep
        push_ref[groups[g][1] + step] = push
        return (product * keep, forward * keep + push, backward + product * push)

    zero = jnp.zeros((SUB, LANES), F32)
    state = {}
    for pair in ((0, 1), (2, 3)):
        for g in pair:
            for load in loads[g]:
                load.wait()
        for g in pair:
            first, _, length = groups[g]
            for row in range(first, first + length * SUB, 16):
                at = pl.ds(row, 16)
                rows_ref[at, :] = signal_ref[at, :].astype(F32) * scale
        state |= all_steps(groups, body, {g: (zero + 1.0, zero, zero) for g in pair})
    ends = []
    for g in range(len(groups)):
        product, forward, backward = state[g]
        whole, forwards = scan_sublanes(product, forward, earlier_sublanes)
        turned, backwards = scan_sublanes(product, backward, later_sublanes)
        parts_ref[4 * g] = whole
        parts_ref[4 * g + 1] = forwards
        parts_ref[4 * g + 2] = turned
        parts_ref[4 * g + 3] = backwards
        ends.append((whole[SUB - 1 :], forwards[SUB - 1 :], backwards[:1]))
    product, forward, backward = ends[0][0], ends[0][1], ends[-1][2]
    for whole, forwards, _ in ends[1:]:
        product, forward = product * whole, forward * whole + forwards
    for whole, _, backwards in reversed(ends[:-1]):
        backward = backwards + whole * backward
    row = lax.broadcasted_iota(jnp.int32, (SUB, LANES), 0)
    packed = jnp.where(row == 0, product, jnp.where(row == 1, forward, backward))
    for copy in range(ends_ref.shape[0]):
        ends_ref[copy] = packed
    parts_ref[4 * len(groups)] = zero + here_ref[0].astype(F32)
    gain_load.wait()


def states_kernel(all_ends_ref, parts_ref, keep_ref, push_ref, states_ref, squares_ref):
    groups = groups_of(keep_ref.shape[0] * SUB)
    here = parts_ref[4 * len(groups), 0:1]
    devices = all_ends_ref.shape[0]
    forward = jnp.zeros((1, LANES), F32)
    backward = jnp.zeros((1, LANES), F32)
    for d in range(devices):
        joined = forward * all_ends_ref[d, 0:1] + all_ends_ref[d, 1:2]
        forward = jnp.where(d < here, joined, forward)
        e = devices - 1 - d
        joined = backward * all_ends_ref[e, 0:1] + all_ends_ref[e, 2:3]
        backward = jnp.where(e > here, joined, backward)

    entering_forward, entering_backward = [], [None] * len(groups)
    for g in range(len(groups)):
        whole, forwards = parts_ref[4 * g], parts_ref[4 * g + 1]
        entering_forward.append(
            earlier_sublanes(forwards, 1, 0.0) + earlier_sublanes(whole, 1, 1.0) * forward
        )
        forward = forwards[SUB - 1 :] + whole[SUB - 1 :] * forward
    for g in reversed(range(len(groups))):
        whole, backwards = parts_ref[4 * g + 2], parts_ref[4 * g + 3]
        entering_backward[g] = (
            later_sublanes(backwards, 1, 0.0) + later_sublanes(whole, 1, 1.0) * backward
        )
        backward = backwards[:1] + whole[:1] * backward

    def forth(g, step, state):
        at = groups[g][1] + step
        state = state * keep_ref[at] + push_ref[at]
        states_ref[at] = state
        return state

    all_steps(groups, forth, dict(enumerate(entering_forward)))
    lane = lax.broadcasted_iota(jnp.int32, (SUB, LANES), 1)
    short = groups[0][2]

    def back(g, step, state):
        state, sums = state
        at = groups[g][1] + step
        state = state * keep_ref[at] + push_ref[at]
        both = states_ref[at] + state
        states_ref[at] = both
        power = jnp.sum(both * both, axis=1, keepdims=True)
        sums = jnp.where(lane == step + (short if g >= 2 else 0), power, sums)
        return state, sums

    zero = jnp.zeros((SUB, LANES), F32)
    done = all_steps(groups, back, {g: (b, zero) for g, b in enumerate(entering_backward)}, reverse=True)
    for half in (0, 1):
        squares = jnp.where(lane < short, done[half][1], done[half + 2][1])
        for copy in range(squares_ref.shape[0]):
            squares_ref[copy, pl.ds(half * SUB, SUB), :] = squares


def norm_kernel(channels, all_squares_ref, states_ref, gain_ref, out_hbm, rows_ref, out_ref, sent):
    groups = groups_of(rows_ref.shape[0])
    short = groups[0][2]
    power = jnp.sum(all_squares_ref[...], axis=0) / channels
    scale = lax.rsqrt(power + 1e-06)
    halves = (scale[:SUB], scale[SUB:])
    gain = jnp.broadcast_to(gain_ref[...], (SUB, LANES))
    stores = []
    for g, (first, at, length) in enumerate(groups):
        for step in range(length):
            lane = step + (short if g >= 2 else 0)
            factor = jnp.broadcast_to(halves[g % 2][:, lane : lane + 1], (SUB, LANES))
            rows_ref[rows_at(groups[g], step), :] = states_ref[at + step] * factor * gain
        for row in range(first, first + length * SUB, 16):
            here = pl.ds(row, 16)
            out_ref[here, :] = rows_ref[here, :].astype(out_ref.dtype)
        rows = rows_of(groups[g])
        stores.append(pltpu.make_async_copy(out_ref.at[rows], out_hbm.at[rows], sent.at[g]))
        stores[-1].start()
    for store in stores:
        store.wait()


def params():
    return pltpu.CompilerParams(vmem_limit_bytes=12 * 1024 * 1024)


def exchanged(x, axis):
    return lax.all_to_all(x, axis, 0, 0, tiled=True)


def per_device(leak_rate, signal_in, norm_gain):
    rows, channels = leak_rate.shape[1], leak_rate.shape[2]
    total_length = rows * lax.axis_size("seq")
    blocks = jax.ShapeDtypeStruct((rows // SUB, SUB, LANES), F32)
    here = lax.axis_index("seq").astype(jnp.int32).reshape(1)
    operands = (leak_rate[0], signal_in[0], norm_gain.reshape(1, channels))
    ends, parts, keep, push, gain = pl.pallas_call(
        functools.partial(summary_kernel, total_length),
        out_shape=(
            jax.ShapeDtypeStruct((lax.axis_size("seq"), SUB, LANES), F32),
            jax.ShapeDtypeStruct((17, SUB, LANES), F32),
            blocks,
            blocks,
            jax.ShapeDtypeStruct((1, LANES), F32),
        ),
        in_specs=[SMEM] + [HBM] * 3,
        out_specs=(VMEM,) * 5,
        scratch_shapes=[
            pltpu.VMEM((rows, LANES), F32),
            pltpu.VMEM((rows, LANES), signal_in.dtype),
            pltpu.VMEM((rows, LANES), F32),
            pltpu.SemaphoreType.DMA((2, 4)),
            pltpu.SemaphoreType.DMA,
        ],
        compiler_params=params(),
        name="summary",
    )(here, *(pltpu.with_memory_space_constraint(x, pltpu.HBM) for x in operands))
    all_ends = exchanged(ends, "seq")
    states, squares = pl.pallas_call(
        states_kernel,
        out_shape=(blocks, jax.ShapeDtypeStruct((lax.axis_size("width"), 2 * SUB, LANES), F32)),
        in_specs=[VMEM] * 4,
        out_specs=(VMEM,) * 2,
        compiler_params=params(),
        name="states",
    )(all_ends, parts, keep, push)
    all_squares = exchanged(squares, "width")
    mixed = pl.pallas_call(
        functools.partial(norm_kernel, channels * lax.axis_size("width")),
        out_shape=jax.ShapeDtypeStruct((rows, LANES), jnp.bfloat16),
        in_specs=[VMEM] * 3,
        out_specs=HBM,
        scratch_shapes=[
            pltpu.VMEM((rows, LANES), F32),
            pltpu.VMEM((rows, LANES), jnp.bfloat16),
            pltpu.SemaphoreType.DMA((4,)),
        ],
        compiler_params=params(),
        name="norm",
    )(all_squares, states, gain)
    return mixed[None]


def solution(mesh):
    return jax.shard_map(
        per_device,
        mesh=mesh,
        in_specs=(P(None, "seq", "width"), P(None, "seq", "width"), P("width")),
        out_specs=P(None, "seq", "width"),
        check_vma=False,
    )
```

```python
import functools

import jax
import jax.numpy as jnp
from jax import lax
from jax.experimental import pallas as pl
from jax.experimental.pallas import tpu as pltpu
from jax.sharding import PartitionSpec as P

LANES = 128
SUB = 8
F32 = jnp.float32
VMEM = pl.BlockSpec(memory_space=pltpu.VMEM)
SMEM = pl.BlockSpec(memory_space=pltpu.SMEM)
HBM = pl.BlockSpec(memory_space=pltpu.HBM)


FIRST = {"seq": 10, "width": 9}


def order_of(axis):
    size = lax.axis_size(axis)
    first = FIRST[axis] % size
    return [first] + [member for member in range(size) if member != first]


def groups_of(rows):
    steps = rows // SUB
    short = steps // 4 - 4
    assert rows % SUB == 0 and short % 8 == 4 and short + 68 <= LANES
    cuts, at = [], 0
    for length in (short, short, short + 8, short + 8):
        cuts.append((at * SUB, at, length))
        at += length
    assert at == steps
    return cuts


def rows_at(group, step):
    first, _, length = group
    return pl.ds(first + step, SUB, stride=length)


def earlier_sublanes(x, by, fill):
    row = lax.broadcasted_iota(jnp.int32, x.shape, 0)
    return jnp.where(row >= by, pltpu.roll(x, by, 0), fill)


def later_sublanes(x, by, fill):
    row = lax.broadcasted_iota(jnp.int32, x.shape, 0)
    return jnp.where(row < SUB - by, pltpu.roll(x, SUB - by, 0), fill)


def scan_sublanes(product, total, shifted):
    for by in (1, 2, 4):
        total = total + product * shifted(total, by, 0.0)
        product = product * shifted(product, by, 1.0)
    return product, total


def all_steps(groups, body, state, reverse=False):
    state = dict(state)
    longest = max(groups[g][2] for g in state)
    for step in reversed(range(longest)) if reverse else range(longest):
        for g in state:
            if step < groups[g][2]:
                state[g] = body(g, step, state[g])
    return state


def rows_of(group):
    first, _, length = group
    return pl.ds(first, length * SUB)


def summary_kernel(
    total_length,
    here_ref,
    leak_hbm,
    signal_hbm,
    gain_hbm,
    ends_ref,
    parts_ref,
    keep_ref,
    push_ref,
    gain_ref,
    leak_ref,
    signal_ref,
    rows_ref,
    arrived,
    gain_arrived,
):
    groups = groups_of(leak_ref.shape[0])
    scale = total_length ** (-0.5)
    loads = []
    for g, group in enumerate(groups):
        at = rows_of(group)
        loads.append(
            (
                pltpu.make_async_copy(leak_hbm.at[at], leak_ref.at[at], arrived.at[0, g]),
                pltpu.make_async_copy(signal_hbm.at[at], signal_ref.at[at], arrived.at[1, g]),
            )
        )
        for load in loads[-1]:
            load.start()
    gain_load = pltpu.make_async_copy(gain_hbm, gain_ref, gain_arrived)
    gain_load.start()

    def body(g, step, state):
        product, forward, backward = state
        keep = jnp.exp(-leak_ref[rows_at(groups[g], step), :] / total_length)
        push = rows_ref[rows_at(groups[g], step), :]
        keep_ref[groups[g][1] + step] = keep
        push_ref[groups[g][1] + step] = push
        return (product * keep, forward * keep + push, backward + product * push)

    zero = jnp.zeros((SUB, LANES), F32)
    state = {}
    for pair in ((0, 1), (2, 3)):
        for g in pair:
            for load in loads[g]:
                load.wait()
        for g in pair:
            first, _, length = groups[g]
            for row in range(first, first + length * SUB, 16):
                at = pl.ds(row, 16)
                rows_ref[at, :] = signal_ref[at, :].astype(F32) * scale
        state |= all_steps(groups, body, {g: (zero + 1.0, zero, zero) for g in pair})
    ends = []
    for g in range(len(groups)):
        product, forward, backward = state[g]
        whole, forwards = scan_sublanes(product, forward, earlier_sublanes)
        turned, backwards = scan_sublanes(product, backward, later_sublanes)
        parts_ref[4 * g] = whole
        parts_ref[4 * g + 1] = forwards
        parts_ref[4 * g + 2] = turned
        parts_ref[4 * g + 3] = backwards
        ends.append((whole[SUB - 1 :], forwards[SUB - 1 :], backwards[:1]))
    product, forward, backward = ends[0][0], ends[0][1], ends[-1][2]
    for whole, forwards, _ in ends[1:]:
        product, forward = product * whole, forward * whole + forwards
    for whole, _, backwards in reversed(ends[:-1]):
        backward = backwards + whole * backward
    row = lax.broadcasted_iota(jnp.int32, (SUB, LANES), 0)
    packed = jnp.where(row == 0, product, jnp.where(row == 1, forward, backward))
    for copy in range(ends_ref.shape[0]):
        ends_ref[copy] = packed
    parts_ref[4 * len(groups)] = zero + here_ref[0].astype(F32)
    gain_load.wait()


def states_kernel(order, all_ends_ref, parts_ref, keep_ref, push_ref, states_ref, squares_ref):
    groups = groups_of(keep_ref.shape[0] * SUB)
    here = parts_ref[4 * len(groups), 0:1]
    devices = len(order)
    place = [order.index(d) for d in range(devices)]
    forward = jnp.zeros((1, LANES), F32)
    backward = jnp.zeros((1, LANES), F32)
    for d in range(devices):
        joined = forward * all_ends_ref[place[d], 0:1] + all_ends_ref[place[d], 1:2]
        forward = jnp.where(d < here, joined, forward)
        e = devices - 1 - d
        joined = backward * all_ends_ref[place[e], 0:1] + all_ends_ref[place[e], 2:3]
        backward = jnp.where(e > here, joined, backward)

    entering_forward, entering_backward = [], [None] * len(groups)
    for g in range(len(groups)):
        whole, forwards = parts_ref[4 * g], parts_ref[4 * g + 1]
        entering_forward.append(
            earlier_sublanes(forwards, 1, 0.0) + earlier_sublanes(whole, 1, 1.0) * forward
        )
        forward = forwards[SUB - 1 :] + whole[SUB - 1 :] * forward
    for g in reversed(range(len(groups))):
        whole, backwards = parts_ref[4 * g + 2], parts_ref[4 * g + 3]
        entering_backward[g] = (
            later_sublanes(backwards, 1, 0.0) + later_sublanes(whole, 1, 1.0) * backward
        )
        backward = backwards[:1] + whole[:1] * backward

    def forth(g, step, state):
        at = groups[g][1] + step
        state = state * keep_ref[at] + push_ref[at]
        states_ref[at] = state
        return state

    all_steps(groups, forth, dict(enumerate(entering_forward)))
    lane = lax.broadcasted_iota(jnp.int32, (SUB, LANES), 1)
    short = groups[0][2]

    def back(g, step, state):
        state, sums = state
        at = groups[g][1] + step
        state = state * keep_ref[at] + push_ref[at]
        both = states_ref[at] + state
        states_ref[at] = both
        power = jnp.sum(both * both, axis=1, keepdims=True)
        sums = jnp.where(lane == step + (short if g >= 2 else 0), power, sums)
        return state, sums

    zero = jnp.zeros((SUB, LANES), F32)
    done = all_steps(groups, back, {g: (b, zero) for g, b in enumerate(entering_backward)}, reverse=True)
    for half in (0, 1):
        squares = jnp.where(lane < short, done[half][1], done[half + 2][1])
        for copy in range(squares_ref.shape[0]):
            squares_ref[copy, pl.ds(half * SUB, SUB), :] = squares


def norm_kernel(channels, all_squares_ref, states_ref, gain_ref, out_hbm, rows_ref, out_ref, sent):
    groups = groups_of(rows_ref.shape[0])
    short = groups[0][2]
    power = jnp.sum(all_squares_ref[...], axis=0) / channels
    scale = lax.rsqrt(power + 1e-06)
    halves = (scale[:SUB], scale[SUB:])
    gain = jnp.broadcast_to(gain_ref[...], (SUB, LANES))
    stores = []
    for g, (first, at, length) in enumerate(groups):
        for step in range(length):
            lane = step + (short if g >= 2 else 0)
            factor = jnp.broadcast_to(halves[g % 2][:, lane : lane + 1], (SUB, LANES))
            rows_ref[rows_at(groups[g], step), :] = states_ref[at + step] * factor * gain
        for row in range(first, first + length * SUB, 16):
            here = pl.ds(row, 16)
            out_ref[here, :] = rows_ref[here, :].astype(out_ref.dtype)
        rows = rows_of(groups[g])
        stores.append(pltpu.make_async_copy(out_ref.at[rows], out_hbm.at[rows], sent.at[g]))
        stores[-1].start()
    for store in stores:
        store.wait()


def params():
    return pltpu.CompilerParams(vmem_limit_bytes=12 * 1024 * 1024)


def exchanged(x, axis):
    return lax.all_to_all(x, axis, 0, 0, tiled=True, axis_index_groups=[order_of(axis)])


def per_device(leak_rate, signal_in, norm_gain):
    rows, channels = leak_rate.shape[1], leak_rate.shape[2]
    total_length = rows * lax.axis_size("seq")
    blocks = jax.ShapeDtypeStruct((rows // SUB, SUB, LANES), F32)
    here = lax.axis_index("seq").astype(jnp.int32).reshape(1)
    operands = (leak_rate[0], signal_in[0], norm_gain.reshape(1, channels))
    ends, parts, keep, push, gain = pl.pallas_call(
        functools.partial(summary_kernel, total_length),
        out_shape=(
            jax.ShapeDtypeStruct((lax.axis_size("seq"), SUB, LANES), F32),
            jax.ShapeDtypeStruct((17, SUB, LANES), F32),
            blocks,
            blocks,
            jax.ShapeDtypeStruct((1, LANES), F32),
        ),
        in_specs=[SMEM] + [HBM] * 3,
        out_specs=(VMEM,) * 5,
        scratch_shapes=[
            pltpu.VMEM((rows, LANES), F32),
            pltpu.VMEM((rows, LANES), signal_in.dtype),
            pltpu.VMEM((rows, LANES), F32),
            pltpu.SemaphoreType.DMA((2, 4)),
            pltpu.SemaphoreType.DMA,
        ],
        compiler_params=params(),
        name="summary",
    )(here, *(pltpu.with_memory_space_constraint(x, pltpu.HBM) for x in operands))
    all_ends = exchanged(ends, "seq")
    states, squares = pl.pallas_call(
        functools.partial(states_kernel, order_of("seq")),
        out_shape=(blocks, jax.ShapeDtypeStruct((lax.axis_size("width"), 2 * SUB, LANES), F32)),
        in_specs=[VMEM] * 4,
        out_specs=(VMEM,) * 2,
        compiler_params=params(),
        name="states",
    )(all_ends, parts, keep, push)
    all_squares = exchanged(squares, "width")
    mixed = pl.pallas_call(
        functools.partial(norm_kernel, channels * lax.axis_size("width")),
        out_shape=jax.ShapeDtypeStruct((rows, LANES), jnp.bfloat16),
        in_specs=[VMEM] * 3,
        out_specs=HBM,
        scratch_shapes=[
            pltpu.VMEM((rows, LANES), F32),
            pltpu.VMEM((rows, LANES), jnp.bfloat16),
            pltpu.SemaphoreType.DMA((4,)),
        ],
        compiler_params=params(),
        name="norm",
    )(all_squares, states, gain)
    return mixed[None]


def solution(mesh):
    return jax.shard_map(
        per_device,
        mesh=mesh,
        in_specs=(P(None, "seq", "width"), P(None, "seq", "width"), P("width")),
        out_specs=P(None, "seq", "width"),
        check_vma=False,
    )
```

```python
import functools

import jax
import jax.numpy as jnp
from jax import lax
from jax.experimental import pallas as pl
from jax.experimental.pallas import tpu as pltpu
from jax.sharding import PartitionSpec as P

LANES = 128
SUB = 8
F32 = jnp.float32
VMEM = pl.BlockSpec(memory_space=pltpu.VMEM)
SMEM = pl.BlockSpec(memory_space=pltpu.SMEM)
HBM = pl.BlockSpec(memory_space=pltpu.HBM)


FAR_STRETCH = 10
FAR_CHIP = 4
CORES = 2


def far_first(members, far):
    return [members[far % len(members)]] + [m for m in members if m != members[far % len(members)]]


def stretches():
    return far_first(list(range(lax.axis_size("seq"))), FAR_STRETCH)


def chips_of_each_core():
    size = lax.axis_size("width")
    return [far_first(list(range(core, size, CORES)), FAR_CHIP) for core in range(CORES)]


def groups_of(rows):
    steps = rows // SUB
    short = steps // 4 - 4
    assert rows % SUB == 0 and short % 8 == 4 and short + 68 <= LANES
    cuts, at = [], 0
    for length in (short, short, short + 8, short + 8):
        cuts.append((at * SUB, at, length))
        at += length
    assert at == steps
    return cuts


def rows_at(group, step):
    first, _, length = group
    return pl.ds(first + step, SUB, stride=length)


def earlier_sublanes(x, by, fill):
    row = lax.broadcasted_iota(jnp.int32, x.shape, 0)
    return jnp.where(row >= by, pltpu.roll(x, by, 0), fill)


def later_sublanes(x, by, fill):
    row = lax.broadcasted_iota(jnp.int32, x.shape, 0)
    return jnp.where(row < SUB - by, pltpu.roll(x, SUB - by, 0), fill)


def scan_sublanes(product, total, shifted):
    for by in (1, 2, 4):
        total = total + product * shifted(total, by, 0.0)
        product = product * shifted(product, by, 1.0)
    return product, total


def all_steps(groups, body, state, reverse=False):
    state = dict(state)
    longest = max(groups[g][2] for g in state)
    for step in reversed(range(longest)) if reverse else range(longest):
        for g in state:
            if step < groups[g][2]:
                state[g] = body(g, step, state[g])
    return state


def rows_of(group):
    first, _, length = group
    return pl.ds(first, length * SUB)


def summary_kernel(
    total_length,
    here_ref,
    leak_hbm,
    signal_hbm,
    gain_hbm,
    ends_ref,
    parts_ref,
    keep_ref,
    push_ref,
    gain_ref,
    leak_ref,
    signal_ref,
    rows_ref,
    arrived,
    gain_arrived,
):
    groups = groups_of(leak_ref.shape[0])
    scale = total_length ** (-0.5)
    loads = []
    for g, group in enumerate(groups):
        at = rows_of(group)
        loads.append(
            (
                pltpu.make_async_copy(leak_hbm.at[at], leak_ref.at[at], arrived.at[0, g]),
                pltpu.make_async_copy(signal_hbm.at[at], signal_ref.at[at], arrived.at[1, g]),
            )
        )
        for load in loads[-1]:
            load.start()
    gain_load = pltpu.make_async_copy(gain_hbm, gain_ref, gain_arrived)
    gain_load.start()

    def body(g, step, state):
        product, forward, backward = state
        keep = jnp.exp(-leak_ref[rows_at(groups[g], step), :] / total_length)
        push = rows_ref[rows_at(groups[g], step), :]
        keep_ref[groups[g][1] + step] = keep
        push_ref[groups[g][1] + step] = push
        return (product * keep, forward * keep + push, backward + product * push)

    zero = jnp.zeros((SUB, LANES), F32)
    state = {}
    for pair in ((0, 1), (2, 3)):
        for g in pair:
            for load in loads[g]:
                load.wait()
        for g in pair:
            first, _, length = groups[g]
            for row in range(first, first + length * SUB, 16):
                at = pl.ds(row, 16)
                rows_ref[at, :] = signal_ref[at, :].astype(F32) * scale
        state |= all_steps(groups, body, {g: (zero + 1.0, zero, zero) for g in pair})
    ends = []
    for g in range(len(groups)):
        product, forward, backward = state[g]
        whole, forwards = scan_sublanes(product, forward, earlier_sublanes)
        turned, backwards = scan_sublanes(product, backward, later_sublanes)
        parts_ref[4 * g] = whole
        parts_ref[4 * g + 1] = forwards
        parts_ref[4 * g + 2] = turned
        parts_ref[4 * g + 3] = backwards
        ends.append((whole[SUB - 1 :], forwards[SUB - 1 :], backwards[:1]))
    product, forward, backward = ends[0][0], ends[0][1], ends[-1][2]
    for whole, forwards, _ in ends[1:]:
        product, forward = product * whole, forward * whole + forwards
    for whole, _, backwards in reversed(ends[:-1]):
        backward = backwards + whole * backward
    row = lax.broadcasted_iota(jnp.int32, (SUB, LANES), 0)
    packed = jnp.where(row == 0, product, jnp.where(row == 1, forward, backward))
    for copy in range(ends_ref.shape[0]):
        ends_ref[copy] = packed[: ends_ref.shape[1]]
    parts_ref[4 * len(groups)] = zero + here_ref[0].astype(F32)
    gain_load.wait()


def states_kernel(order, all_ends_ref, parts_ref, keep_ref, push_ref, states_ref, squares_ref):
    groups = groups_of(keep_ref.shape[0] * SUB)
    here = parts_ref[4 * len(groups), 0:1]
    devices = len(order)
    place = [order.index(d) for d in range(devices)]
    forward = jnp.zeros((1, LANES), F32)
    backward = jnp.zeros((1, LANES), F32)
    for d in range(devices):
        joined = forward * all_ends_ref[place[d], 0:1] + all_ends_ref[place[d], 1:2]
        forward = jnp.where(d < here, joined, forward)
        e = devices - 1 - d
        joined = backward * all_ends_ref[place[e], 0:1] + all_ends_ref[place[e], 2:3]
        backward = jnp.where(e > here, joined, backward)

    entering_forward, entering_backward = [], [None] * len(groups)
    for g in range(len(groups)):
        whole, forwards = parts_ref[4 * g], parts_ref[4 * g + 1]
        entering_forward.append(
            earlier_sublanes(forwards, 1, 0.0) + earlier_sublanes(whole, 1, 1.0) * forward
        )
        forward = forwards[SUB - 1 :] + whole[SUB - 1 :] * forward
    for g in reversed(range(len(groups))):
        whole, backwards = parts_ref[4 * g + 2], parts_ref[4 * g + 3]
        entering_backward[g] = (
            later_sublanes(backwards, 1, 0.0) + later_sublanes(whole, 1, 1.0) * backward
        )
        backward = backwards[:1] + whole[:1] * backward

    def forth(g, step, state):
        at = groups[g][1] + step
        state = state * keep_ref[at] + push_ref[at]
        states_ref[at] = state
        return state

    all_steps(groups, forth, dict(enumerate(entering_forward)))
    lane = lax.broadcasted_iota(jnp.int32, (SUB, LANES), 1)
    short = groups[0][2]

    def back(g, step, state):
        state, sums = state
        at = groups[g][1] + step
        state = state * keep_ref[at] + push_ref[at]
        both = states_ref[at] + state
        states_ref[at] = both
        power = jnp.sum(both * both, axis=1, keepdims=True)
        sums = jnp.where(lane == step + (short if g >= 2 else 0), power, sums)
        return state, sums

    zero = jnp.zeros((SUB, LANES), F32)
    done = all_steps(groups, back, {g: (b, zero) for g, b in enumerate(entering_backward)}, reverse=True)
    for half in (0, 1):
        squares = jnp.where(lane < short, done[half][1], done[half + 2][1])
        squares_ref[pl.ds(half * SUB, SUB), :] = squares


def norm_kernel(channels, all_squares_ref, states_ref, gain_ref, out_hbm, rows_ref, out_ref, sent):
    groups = groups_of(rows_ref.shape[0])
    short = groups[0][2]
    power = jnp.sum(all_squares_ref[...], axis=0) / channels
    scale = lax.rsqrt(power + 1e-06)
    halves = (scale[:SUB], scale[SUB:])
    gain = jnp.broadcast_to(gain_ref[...], (SUB, LANES))
    stores = []
    for g, (first, at, length) in enumerate(groups):
        for step in range(length):
            lane = step + (short if g >= 2 else 0)
            factor = jnp.broadcast_to(halves[g % 2][:, lane : lane + 1], (SUB, LANES))
            rows_ref[rows_at(groups[g], step), :] = states_ref[at + step] * factor * gain
        for row in range(first, first + length * SUB, 16):
            here = pl.ds(row, 16)
            out_ref[here, :] = rows_ref[here, :].astype(out_ref.dtype)
        rows = rows_of(groups[g])
        stores.append(pltpu.make_async_copy(out_ref.at[rows], out_hbm.at[rows], sent.at[g]))
        stores[-1].start()
    for store in stores:
        store.wait()


def params():
    return pltpu.CompilerParams(vmem_limit_bytes=12 * 1024 * 1024)


def exchanged(x, axis, groups):
    return lax.all_to_all(x, axis, 0, 0, tiled=True, axis_index_groups=groups)


def per_device(leak_rate, signal_in, norm_gain):
    rows, channels = leak_rate.shape[1], leak_rate.shape[2]
    total_length = rows * lax.axis_size("seq")
    blocks = jax.ShapeDtypeStruct((rows // SUB, SUB, LANES), F32)
    here = lax.axis_index("seq").astype(jnp.int32).reshape(1)
    operands = (leak_rate[0], signal_in[0], norm_gain.reshape(1, channels))
    ends, parts, keep, push, gain = pl.pallas_call(
        functools.partial(summary_kernel, total_length),
        out_shape=(
            jax.ShapeDtypeStruct((lax.axis_size("seq"), 4, LANES), F32),
            jax.ShapeDtypeStruct((17, SUB, LANES), F32),
            blocks,
            blocks,
            jax.ShapeDtypeStruct((1, LANES), F32),
        ),
        in_specs=[SMEM] + [HBM] * 3,
        out_specs=(VMEM,) * 5,
        scratch_shapes=[
            pltpu.VMEM((rows, LANES), F32),
            pltpu.VMEM((rows, LANES), signal_in.dtype),
            pltpu.VMEM((rows, LANES), F32),
            pltpu.SemaphoreType.DMA((2, 4)),
            pltpu.SemaphoreType.DMA,
        ],
        compiler_params=params(),
        name="summary",
    )(here, *(pltpu.with_memory_space_constraint(x, pltpu.HBM) for x in operands))
    all_ends = exchanged(ends, "seq", [stretches()])
    states, squares = pl.pallas_call(
        functools.partial(states_kernel, stretches()),
        out_shape=(blocks, jax.ShapeDtypeStruct((2 * SUB, LANES), F32)),
        in_specs=[VMEM] * 4,
        out_specs=(VMEM,) * 2,
        compiler_params=params(),
        name="states",
    )(all_ends, parts, keep, push)
    width = lax.axis_size("width")
    partners = [(member, member ^ 1) for member in range(width)]
    squares = squares + lax.ppermute(squares, "width", partners)
    squares = jnp.broadcast_to(squares[None], (width // CORES, *squares.shape))
    all_squares = exchanged(squares, "width", chips_of_each_core())
    mixed = pl.pallas_call(
        functools.partial(norm_kernel, channels * lax.axis_size("width")),
        out_shape=jax.ShapeDtypeStruct((rows, LANES), jnp.bfloat16),
        in_specs=[VMEM] * 3,
        out_specs=HBM,
        scratch_shapes=[
            pltpu.VMEM((rows, LANES), F32),
            pltpu.VMEM((rows, LANES), jnp.bfloat16),
            pltpu.SemaphoreType.DMA((4,)),
        ],
        compiler_params=params(),
        name="norm",
    )(all_squares, states, gain)
    return mixed[None]


def solution(mesh):
    return jax.shard_map(
        per_device,
        mesh=mesh,
        in_specs=(P(None, "seq", "width"), P(None, "seq", "width"), P("width")),
        out_specs=P(None, "seq", "width"),
        check_vma=False,
    )
```

```python
import functools
import math

import jax
import jax.numpy as jnp
from jax import lax
from jax.experimental import pallas as pl
from jax.experimental.pallas import tpu as pltpu
from jax.sharding import PartitionSpec as P

LANES = 128
SUB = 8
F32 = jnp.float32
VMEM = pl.BlockSpec(memory_space=pltpu.VMEM)
SMEM = pl.BlockSpec(memory_space=pltpu.SMEM)
HBM = pl.BlockSpec(memory_space=pltpu.HBM)


FAR_STRETCH = 10
FAR_CHIP = 4
CORES = 2


def far_first(members, far):
    return [members[far % len(members)]] + [m for m in members if m != members[far % len(members)]]


def stretches():
    return far_first(list(range(lax.axis_size("seq"))), FAR_STRETCH)


def chips_of_each_core():
    size = lax.axis_size("width")
    return [far_first(list(range(core, size, CORES)), FAR_CHIP) for core in range(CORES)]


def groups_of(rows):
    steps = rows // SUB
    short = steps // 4 - 4
    assert rows % SUB == 0 and short % 8 == 4 and short + 68 <= LANES
    cuts, at = [], 0
    for length in (short, short, short + 8, short + 8):
        cuts.append((at * SUB, at, length))
        at += length
    assert at == steps
    return cuts


def rows_at(group, step):
    first, _, length = group
    return pl.ds(first + step, SUB, stride=length)


def earlier_sublanes(x, by, fill):
    row = lax.broadcasted_iota(jnp.int32, x.shape, 0)
    return jnp.where(row >= by, pltpu.roll(x, by, 0), fill)


def later_sublanes(x, by, fill):
    row = lax.broadcasted_iota(jnp.int32, x.shape, 0)
    return jnp.where(row < SUB - by, pltpu.roll(x, SUB - by, 0), fill)


def scan_sublanes(product, total, shifted):
    for by in (1, 2, 4):
        total = total + product * shifted(total, by, 0.0)
        product = product * shifted(product, by, 1.0)
    return product, total


def all_steps(groups, body, state, reverse=False):
    state = dict(state)
    longest = max(groups[g][2] for g in state)
    for step in reversed(range(longest)) if reverse else range(longest):
        for g in state:
            if step < groups[g][2]:
                state[g] = body(g, step, state[g])
    return state


def rows_of(groups, cut):
    return pl.ds(groups[cut[0]][0], sum(groups[g][2] for g in cut) * SUB)


def summary_kernel(
    total_length,
    here_ref,
    leak_hbm,
    signal_hbm,
    gain_hbm,
    ends_ref,
    parts_ref,
    keep_ref,
    push_ref,
    gain_ref,
    leak_ref,
    signal_ref,
    rows_ref,
    arrived,
    gain_arrived,
):
    groups = groups_of(leak_ref.shape[0])
    scale = total_length ** (-0.5)
    exponent = -math.log2(math.e) / total_length
    halves = ((0, 1), (2, 3))
    signal_load = pltpu.make_async_copy(signal_hbm, signal_ref, arrived.at[0])
    signal_load.start()
    leak_loads = []
    for half, cut in enumerate(halves):
        at = rows_of(groups, cut)
        leak_loads.append(pltpu.make_async_copy(leak_hbm.at[at], leak_ref.at[at], arrived.at[1 + half]))
        leak_loads[-1].start()
    gain_load = pltpu.make_async_copy(gain_hbm, gain_ref, gain_arrived)
    gain_load.start()

    def body(g, step, state):
        product, forward, backward = state
        keep = jnp.exp2(leak_ref[rows_at(groups[g], step), :] * exponent)
        push = rows_ref[rows_at(groups[g], step), :]
        keep_ref[groups[g][1] + step] = keep
        push_ref[groups[g][1] + step] = push
        return (product * keep, forward * keep + push, backward + product * push)

    zero = jnp.zeros((SUB, LANES), F32)
    state = {}
    signal_load.wait()
    for row in range(0, leak_ref.shape[0], 16):
        at = pl.ds(row, 16)
        rows_ref[at, :] = signal_ref[at, :].astype(F32) * scale
    for cut, load in zip(halves, leak_loads):
        load.wait()
        state |= all_steps(groups, body, {g: (zero + 1.0, zero, zero) for g in cut})
    ends = []
    for g in range(len(groups)):
        product, forward, backward = state[g]
        whole, forwards = scan_sublanes(product, forward, earlier_sublanes)
        turned, backwards = scan_sublanes(product, backward, later_sublanes)
        parts_ref[4 * g] = whole
        parts_ref[4 * g + 1] = forwards
        parts_ref[4 * g + 2] = turned
        parts_ref[4 * g + 3] = backwards
        ends.append((whole[SUB - 1 :], forwards[SUB - 1 :], backwards[:1]))
    product, forward, backward = ends[0][0], ends[0][1], ends[-1][2]
    for whole, forwards, _ in ends[1:]:
        product, forward = product * whole, forward * whole + forwards
    for whole, _, backwards in reversed(ends[:-1]):
        backward = backwards + whole * backward
    row = lax.broadcasted_iota(jnp.int32, (SUB, LANES), 0)
    packed = jnp.where(row == 0, product, jnp.where(row == 1, forward, backward))
    for copy in range(ends_ref.shape[0]):
        ends_ref[copy] = packed[: ends_ref.shape[1]]
    parts_ref[4 * len(groups)] = zero + here_ref[0].astype(F32)
    gain_load.wait()


def states_kernel(order, all_ends_ref, parts_ref, keep_ref, push_ref, states_ref, squares_ref):
    groups = groups_of(keep_ref.shape[0] * SUB)
    here = parts_ref[4 * len(groups), 0:1]
    devices = len(order)
    place = [order.index(d) for d in range(devices)]
    forward = jnp.zeros((1, LANES), F32)
    backward = jnp.zeros((1, LANES), F32)
    for d in range(devices):
        joined = forward * all_ends_ref[place[d], 0:1] + all_ends_ref[place[d], 1:2]
        forward = jnp.where(d < here, joined, forward)
        e = devices - 1 - d
        joined = backward * all_ends_ref[place[e], 0:1] + all_ends_ref[place[e], 2:3]
        backward = jnp.where(e > here, joined, backward)

    entering_forward, entering_backward = [], [None] * len(groups)
    for g in range(len(groups)):
        whole, forwards = parts_ref[4 * g], parts_ref[4 * g + 1]
        entering_forward.append(
            earlier_sublanes(forwards, 1, 0.0) + earlier_sublanes(whole, 1, 1.0) * forward
        )
        forward = forwards[SUB - 1 :] + whole[SUB - 1 :] * forward
    for g in reversed(range(len(groups))):
        whole, backwards = parts_ref[4 * g + 2], parts_ref[4 * g + 3]
        entering_backward[g] = (
            later_sublanes(backwards, 1, 0.0) + later_sublanes(whole, 1, 1.0) * backward
        )
        backward = backwards[:1] + whole[:1] * backward

    def forth(g, step, state):
        at = groups[g][1] + step
        state = state * keep_ref[at] + push_ref[at]
        states_ref[at] = state
        return state

    all_steps(groups, forth, dict(enumerate(entering_forward)))
    lane = lax.broadcasted_iota(jnp.int32, (SUB, LANES), 1)
    short = groups[0][2]

    def back(g, step, state):
        state, sums = state
        at = groups[g][1] + step
        state = state * keep_ref[at] + push_ref[at]
        both = states_ref[at] + state
        states_ref[at] = both
        power = jnp.sum(both * both, axis=1, keepdims=True)
        sums = jnp.where(lane == step + (short if g >= 2 else 0), power, sums)
        return state, sums

    zero = jnp.zeros((SUB, LANES), F32)
    done = all_steps(groups, back, {g: (b, zero) for g, b in enumerate(entering_backward)}, reverse=True)
    for half in (0, 1):
        squares = jnp.where(lane < short, done[half][1], done[half + 2][1])
        squares_ref[pl.ds(half * SUB, SUB), :] = squares


def norm_kernel(channels, all_squares_ref, states_ref, gain_ref, out_hbm, rows_ref, out_ref, sent):
    groups = groups_of(rows_ref.shape[0])
    short = groups[0][2]
    power = jnp.sum(all_squares_ref[...], axis=0) / channels
    scale = lax.rsqrt(power + 1e-06)
    halves = (scale[:SUB], scale[SUB:])
    gain = jnp.broadcast_to(gain_ref[...], (SUB, LANES))
    lanes = lax.broadcasted_iota(jnp.int32, (SUB, LANES), 1)
    stores = []
    for g, (first, at, length) in enumerate(groups):
        for step in range(length):
            lane = step + (short if g >= 2 else 0)
            factor = jnp.sum(jnp.where(lanes == lane, halves[g % 2], 0.0), axis=1, keepdims=True)
            rows_ref[rows_at(groups[g], step), :] = states_ref[at + step] * factor * gain
        for row in range(first, first + length * SUB, 16):
            here = pl.ds(row, 16)
            out_ref[here, :] = rows_ref[here, :].astype(out_ref.dtype)
        if g % 2:
            rows = rows_of(groups, (g - 1, g))
            stores.append(pltpu.make_async_copy(out_ref.at[rows], out_hbm.at[rows], sent.at[g // 2]))
            stores[-1].start()
    for store in stores:
        store.wait()


def params():
    return pltpu.CompilerParams(vmem_limit_bytes=12 * 1024 * 1024)


def exchanged(x, axis, groups):
    return lax.all_to_all(x, axis, 0, 0, tiled=True, axis_index_groups=groups)


def per_device(leak_rate, signal_in, norm_gain):
    rows, channels = leak_rate.shape[1], leak_rate.shape[2]
    total_length = rows * lax.axis_size("seq")
    blocks = jax.ShapeDtypeStruct((rows // SUB, SUB, LANES), F32)
    here = lax.axis_index("seq").astype(jnp.int32).reshape(1)
    operands = (leak_rate[0], signal_in[0], norm_gain.reshape(1, channels))
    ends, parts, keep, push, gain = pl.pallas_call(
        functools.partial(summary_kernel, total_length),
        out_shape=(
            jax.ShapeDtypeStruct((lax.axis_size("seq"), 4, LANES), F32),
            jax.ShapeDtypeStruct((17, SUB, LANES), F32),
            blocks,
            blocks,
            jax.ShapeDtypeStruct((1, LANES), F32),
        ),
        in_specs=[SMEM] + [HBM] * 3,
        out_specs=(VMEM,) * 5,
        scratch_shapes=[
            pltpu.VMEM((rows, LANES), F32),
            pltpu.VMEM((rows, LANES), signal_in.dtype),
            pltpu.VMEM((rows, LANES), F32),
            pltpu.SemaphoreType.DMA((3,)),
            pltpu.SemaphoreType.DMA,
        ],
        compiler_params=params(),
        name="summary",
    )(here, *(pltpu.with_memory_space_constraint(x, pltpu.HBM) for x in operands))
    all_ends = exchanged(ends, "seq", [stretches()])
    states, squares = pl.pallas_call(
        functools.partial(states_kernel, stretches()),
        out_shape=(blocks, jax.ShapeDtypeStruct((2 * SUB, LANES), F32)),
        in_specs=[VMEM] * 4,
        out_specs=(VMEM,) * 2,
        compiler_params=params(),
        name="states",
    )(all_ends, parts, keep, push)
    width = lax.axis_size("width")
    partners = [(member, member ^ 1) for member in range(width)]
    squares = squares + lax.ppermute(squares, "width", partners)
    squares = jnp.broadcast_to(squares[None], (width // CORES, *squares.shape))
    all_squares = exchanged(squares, "width", chips_of_each_core())
    mixed = pl.pallas_call(
        functools.partial(norm_kernel, channels * lax.axis_size("width")),
        out_shape=jax.ShapeDtypeStruct((rows, LANES), jnp.bfloat16),
        in_specs=[VMEM] * 3,
        out_specs=HBM,
        scratch_shapes=[
            pltpu.VMEM((rows, LANES), F32),
            pltpu.VMEM((rows, LANES), jnp.bfloat16),
            pltpu.SemaphoreType.DMA((2,)),
        ],
        compiler_params=params(),
        name="norm",
    )(all_squares, states, gain)
    return mixed[None]


def solution(mesh):
    return jax.shard_map(
        per_device,
        mesh=mesh,
        in_specs=(P(None, "seq", "width"), P(None, "seq", "width"), P("width")),
        out_specs=P(None, "seq", "width"),
        check_vma=False,
    )
```

```python
import functools
import math

import jax
import jax.numpy as jnp
from jax import lax
from jax.experimental import pallas as pl
from jax.experimental.pallas import tpu as pltpu
from jax.sharding import PartitionSpec as P

LANES = 128
SUB = 8
F32 = jnp.float32
VMEM = pl.BlockSpec(memory_space=pltpu.VMEM)
SMEM = pl.BlockSpec(memory_space=pltpu.SMEM)
HBM = pl.BlockSpec(memory_space=pltpu.HBM)


FAR_STRETCH = 10
FAR_CHIP = 4
CORES = 2


def far_first(members, far):
    return [members[far % len(members)]] + [m for m in members if m != members[far % len(members)]]


def stretches():
    return far_first(list(range(lax.axis_size("seq"))), FAR_STRETCH)


def chips_of_each_core():
    size = lax.axis_size("width")
    return [far_first(list(range(core, size, CORES)), FAR_CHIP) for core in range(CORES)]


def groups_of(rows):
    steps = rows // SUB
    short = steps // 4 - 4
    assert rows % SUB == 0 and short % 8 == 4 and short + 68 <= LANES
    cuts, at = [], 0
    for length in (short, short, short + 8, short + 8):
        cuts.append((at * SUB, at, length))
        at += length
    assert at == steps
    return cuts


def rows_at(group, step):
    first, _, length = group
    return pl.ds(first + step, SUB, stride=length)


def earlier_sublanes(x, by, fill):
    row = lax.broadcasted_iota(jnp.int32, x.shape, 0)
    return jnp.where(row >= by, pltpu.roll(x, by, 0), fill)


def later_sublanes(x, by, fill):
    row = lax.broadcasted_iota(jnp.int32, x.shape, 0)
    return jnp.where(row < SUB - by, pltpu.roll(x, SUB - by, 0), fill)


def scan_sublanes(product, total, shifted):
    for by in (1, 2, 4):
        total = total + product * shifted(total, by, 0.0)
        product = product * shifted(product, by, 1.0)
    return product, total


def all_steps(groups, body, state, reverse=False):
    state = dict(state)
    longest = max(groups[g][2] for g in state)
    for step in reversed(range(longest)) if reverse else range(longest):
        for g in state:
            if step < groups[g][2]:
                state[g] = body(g, step, state[g])
    return state


def rows_of(groups, cut):
    return pl.ds(groups[cut[0]][0], sum(groups[g][2] for g in cut) * SUB)


def summary_kernel(
    total_length,
    here_ref,
    leak_hbm,
    signal_hbm,
    gain_hbm,
    ends_ref,
    parts_ref,
    keep_ref,
    push_ref,
    product_ref,
    forward_ref,
    gain_ref,
    leak_ref,
    signal_ref,
    rows_ref,
    arrived,
    gain_arrived,
):
    groups = groups_of(leak_ref.shape[0])
    scale = total_length ** (-0.5)
    exponent = -math.log2(math.e) / total_length
    halves = ((0, 1), (2, 3))
    signal_load = pltpu.make_async_copy(signal_hbm, signal_ref, arrived.at[0])
    signal_load.start()
    leak_loads = []
    for half, cut in enumerate(halves):
        at = rows_of(groups, cut)
        leak_loads.append(pltpu.make_async_copy(leak_hbm.at[at], leak_ref.at[at], arrived.at[1 + half]))
        leak_loads[-1].start()
    gain_load = pltpu.make_async_copy(gain_hbm, gain_ref, gain_arrived)
    gain_load.start()

    def body(g, step, state):
        product, forward, backward = state
        keep = jnp.exp2(leak_ref[rows_at(groups[g], step), :] * exponent)
        push = rows_ref[rows_at(groups[g], step), :]
        keep_ref[groups[g][1] + step] = keep
        push_ref[groups[g][1] + step] = push
        backward = backward + product * push
        product, forward = product * keep, forward * keep + push
        product_ref[groups[g][1] + step] = product
        forward_ref[groups[g][1] + step] = forward
        return (product, forward, backward)

    zero = jnp.zeros((SUB, LANES), F32)
    state = {}
    signal_load.wait()
    for row in range(0, leak_ref.shape[0], 16):
        at = pl.ds(row, 16)
        rows_ref[at, :] = signal_ref[at, :].astype(F32) * scale
    for cut, load in zip(halves, leak_loads):
        load.wait()
        state |= all_steps(groups, body, {g: (zero + 1.0, zero, zero) for g in cut})
    ends = []
    for g in range(len(groups)):
        product, forward, backward = state[g]
        whole, forwards = scan_sublanes(product, forward, earlier_sublanes)
        turned, backwards = scan_sublanes(product, backward, later_sublanes)
        parts_ref[4 * g] = whole
        parts_ref[4 * g + 1] = forwards
        parts_ref[4 * g + 2] = turned
        parts_ref[4 * g + 3] = backwards
        ends.append((whole[SUB - 1 :], forwards[SUB - 1 :], backwards[:1]))
    product, forward, backward = ends[0][0], ends[0][1], ends[-1][2]
    for whole, forwards, _ in ends[1:]:
        product, forward = product * whole, forward * whole + forwards
    for whole, _, backwards in reversed(ends[:-1]):
        backward = backwards + whole * backward
    row = lax.broadcasted_iota(jnp.int32, (SUB, LANES), 0)
    packed = jnp.where(row == 0, product, jnp.where(row == 1, forward, backward))
    for copy in range(ends_ref.shape[0]):
        ends_ref[copy] = packed[: ends_ref.shape[1]]
    parts_ref[4 * len(groups)] = zero + here_ref[0].astype(F32)
    gain_load.wait()


def states_kernel(
    order,
    all_ends_ref,
    parts_ref,
    keep_ref,
    push_ref,
    product_ref,
    forward_ref,
    gain_ref,
    states_ref,
    squares_ref,
):
    groups = groups_of(keep_ref.shape[0] * SUB)
    here = parts_ref[4 * len(groups), 0:1]
    devices = len(order)
    place = [order.index(d) for d in range(devices)]
    forward = jnp.zeros((1, LANES), F32)
    backward = jnp.zeros((1, LANES), F32)
    for d in range(devices):
        joined = forward * all_ends_ref[place[d], 0:1] + all_ends_ref[place[d], 1:2]
        forward = jnp.where(d < here, joined, forward)
        e = devices - 1 - d
        joined = backward * all_ends_ref[place[e], 0:1] + all_ends_ref[place[e], 2:3]
        backward = jnp.where(e > here, joined, backward)

    entering_forward, entering_backward = [], [None] * len(groups)
    for g in range(len(groups)):
        whole, forwards = parts_ref[4 * g], parts_ref[4 * g + 1]
        entering_forward.append(
            earlier_sublanes(forwards, 1, 0.0) + earlier_sublanes(whole, 1, 1.0) * forward
        )
        forward = forwards[SUB - 1 :] + whole[SUB - 1 :] * forward
    for g in reversed(range(len(groups))):
        whole, backwards = parts_ref[4 * g + 2], parts_ref[4 * g + 3]
        entering_backward[g] = (
            later_sublanes(backwards, 1, 0.0) + later_sublanes(whole, 1, 1.0) * backward
        )
        backward = backwards[:1] + whole[:1] * backward

    gain = jnp.broadcast_to(gain_ref[...], (SUB, LANES))
    lane = lax.broadcasted_iota(jnp.int32, (SUB, LANES), 1)
    short = groups[0][2]

    def back(g, step, state):
        state, sums = state
        at = groups[g][1] + step
        state = state * keep_ref[at] + push_ref[at]
        both = (forward_ref[at] + product_ref[at] * entering_forward[g]) + state
        states_ref[at] = both * gain
        power = jnp.sum(both * both, axis=1, keepdims=True)
        sums = jnp.where(lane == step + (short if g >= 2 else 0), power, sums)
        return state, sums

    zero = jnp.zeros((SUB, LANES), F32)
    done = all_steps(groups, back, {g: (b, zero) for g, b in enumerate(entering_backward)}, reverse=True)
    for half in (0, 1):
        squares = jnp.where(lane < short, done[half][1], done[half + 2][1])
        squares_ref[pl.ds(half * SUB, SUB), :] = squares


def norm_kernel(channels, all_squares_ref, states_ref, out_hbm, rows_ref, out_ref, sent):
    groups = groups_of(rows_ref.shape[0])
    short = groups[0][2]
    power = jnp.sum(all_squares_ref[...], axis=0) / channels
    scale = lax.rsqrt(power + 1e-06)
    halves = (scale[:SUB], scale[SUB:])
    lanes = lax.broadcasted_iota(jnp.int32, (SUB, LANES), 1)
    stores = []
    for g, (first, at, length) in enumerate(groups):
        for step in range(length):
            lane = step + (short if g >= 2 else 0)
            factor = jnp.sum(jnp.where(lanes == lane, halves[g % 2], 0.0), axis=1, keepdims=True)
            rows_ref[rows_at(groups[g], step), :] = states_ref[at + step] * factor
        for row in range(first, first + length * SUB, 16):
            here = pl.ds(row, 16)
            out_ref[here, :] = rows_ref[here, :].astype(out_ref.dtype)
        if g % 2:
            rows = rows_of(groups, (g - 1, g))
            stores.append(pltpu.make_async_copy(out_ref.at[rows], out_hbm.at[rows], sent.at[g // 2]))
            stores[-1].start()
    for store in stores:
        store.wait()


def params():
    return pltpu.CompilerParams(vmem_limit_bytes=12 * 1024 * 1024)


def exchanged(x, axis, groups):
    return lax.all_to_all(x, axis, 0, 0, tiled=True, axis_index_groups=groups)


def per_device(leak_rate, signal_in, norm_gain):
    rows, channels = leak_rate.shape[1], leak_rate.shape[2]
    total_length = rows * lax.axis_size("seq")
    blocks = jax.ShapeDtypeStruct((rows // SUB, SUB, LANES), F32)
    here = lax.axis_index("seq").astype(jnp.int32).reshape(1)
    operands = (leak_rate[0], signal_in[0], norm_gain.reshape(1, channels))
    ends, *scanned = pl.pallas_call(
        functools.partial(summary_kernel, total_length),
        out_shape=(
            jax.ShapeDtypeStruct((lax.axis_size("seq"), 4, LANES), F32),
            jax.ShapeDtypeStruct((17, SUB, LANES), F32),
            blocks,
            blocks,
            blocks,
            blocks,
            jax.ShapeDtypeStruct((1, LANES), F32),
        ),
        in_specs=[SMEM] + [HBM] * 3,
        out_specs=(VMEM,) * 7,
        scratch_shapes=[
            pltpu.VMEM((rows, LANES), F32),
            pltpu.VMEM((rows, LANES), signal_in.dtype),
            pltpu.VMEM((rows, LANES), F32),
            pltpu.SemaphoreType.DMA((3,)),
            pltpu.SemaphoreType.DMA,
        ],
        compiler_params=params(),
        name="summary",
    )(here, *(pltpu.with_memory_space_constraint(x, pltpu.HBM) for x in operands))
    all_ends = exchanged(ends, "seq", [stretches()])
    states, squares = pl.pallas_call(
        functools.partial(states_kernel, stretches()),
        out_shape=(blocks, jax.ShapeDtypeStruct((2 * SUB, LANES), F32)),
        in_specs=[VMEM] * 7,
        out_specs=(VMEM,) * 2,
        compiler_params=params(),
        name="states",
    )(all_ends, *scanned)
    width = lax.axis_size("width")
    partners = [(member, member ^ 1) for member in range(width)]
    squares = squares + lax.ppermute(squares, "width", partners)
    squares = jnp.broadcast_to(squares[None], (width // CORES, *squares.shape))
    all_squares = exchanged(squares, "width", chips_of_each_core())
    mixed = pl.pallas_call(
        functools.partial(norm_kernel, channels * lax.axis_size("width")),
        out_shape=jax.ShapeDtypeStruct((rows, LANES), jnp.bfloat16),
        in_specs=[VMEM] * 2,
        out_specs=HBM,
        scratch_shapes=[
            pltpu.VMEM((rows, LANES), F32),
            pltpu.VMEM((rows, LANES), jnp.bfloat16),
            pltpu.SemaphoreType.DMA((2,)),
        ],
        compiler_params=params(),
        name="norm",
    )(all_squares, states)
    return mixed[None]


def solution(mesh):
    return jax.shard_map(
        per_device,
        mesh=mesh,
        in_specs=(P(None, "seq", "width"), P(None, "seq", "width"), P("width")),
        out_specs=P(None, "seq", "width"),
        check_vma=False,
    )
```

```python
import functools
import math

import jax
import jax.numpy as jnp
from jax import lax
from jax.experimental import pallas as pl
from jax.experimental.pallas import tpu as pltpu
from jax.sharding import PartitionSpec as P

LANES = 128
SUB = 8
F32 = jnp.float32
VMEM = pl.BlockSpec(memory_space=pltpu.VMEM)
SMEM = pl.BlockSpec(memory_space=pltpu.SMEM)
HBM = pl.BlockSpec(memory_space=pltpu.HBM)


FAR_STRETCH = 10
FAR_CHIP = 4
CORES = 2


def far_first(members, far):
    return [members[far % len(members)]] + [m for m in members if m != members[far % len(members)]]


def stretches():
    return far_first(list(range(lax.axis_size("seq"))), FAR_STRETCH)


def chips_of_each_core():
    size = lax.axis_size("width")
    return [far_first(list(range(core, size, CORES)), FAR_CHIP) for core in range(CORES)]


def groups_of(rows):
    steps = rows // SUB
    short = steps // 4 - 4
    assert rows % SUB == 0 and short % 8 == 4 and short + 68 <= LANES
    cuts, at = [], 0
    for length in (short + 8, short + 8, short, short):
        cuts.append((at * SUB, at, length))
        at += length
    assert at == steps
    return cuts


def rows_at(group, step):
    first, _, length = group
    return pl.ds(first + step, SUB, stride=length)


def earlier_sublanes(x, by, fill):
    row = lax.broadcasted_iota(jnp.int32, x.shape, 0)
    return jnp.where(row >= by, pltpu.roll(x, by, 0), fill)


def later_sublanes(x, by, fill):
    row = lax.broadcasted_iota(jnp.int32, x.shape, 0)
    return jnp.where(row < SUB - by, pltpu.roll(x, SUB - by, 0), fill)


def scan_sublanes(product, total, shifted):
    for by in (1, 2, 4):
        total = total + product * shifted(total, by, 0.0)
        product = product * shifted(product, by, 1.0)
    return product, total


def all_steps(groups, body, state, reverse=False):
    state = dict(state)
    longest = max(groups[g][2] for g in state)
    for step in reversed(range(longest)) if reverse else range(longest):
        for g in state:
            if step < groups[g][2]:
                state[g] = body(g, step, state[g])
    return state


def rows_of(groups, cut):
    return pl.ds(groups[cut[0]][0], sum(groups[g][2] for g in cut) * SUB)


def summary_kernel(
    total_length,
    here_ref,
    leak_hbm,
    signal_hbm,
    gain_hbm,
    ends_ref,
    parts_ref,
    keep_ref,
    push_ref,
    product_ref,
    forward_ref,
    gain_ref,
    leak_ref,
    signal_ref,
    rows_ref,
    arrived,
    gain_arrived,
):
    groups = groups_of(leak_ref.shape[0])
    scale = total_length ** (-0.5)
    exponent = -math.log2(math.e) / total_length
    halves = ((0, 1), (2, 3))
    signal_load = pltpu.make_async_copy(signal_hbm, signal_ref, arrived.at[0])
    signal_load.start()
    leak_loads = []
    for half, cut in enumerate(halves):
        at = rows_of(groups, cut)
        leak_loads.append(pltpu.make_async_copy(leak_hbm.at[at], leak_ref.at[at], arrived.at[1 + half]))
        leak_loads[-1].start()
    gain_load = pltpu.make_async_copy(gain_hbm, gain_ref, gain_arrived)
    gain_load.start()

    def body(g, step, state):
        product, forward, backward = state
        keep = jnp.exp2(leak_ref[rows_at(groups[g], step), :] * exponent)
        push = rows_ref[rows_at(groups[g], step), :]
        keep_ref[groups[g][1] + step] = keep
        push_ref[groups[g][1] + step] = push
        backward = backward + product * push
        product, forward = product * keep, forward * keep + push
        product_ref[groups[g][1] + step] = product
        forward_ref[groups[g][1] + step] = forward
        return (product, forward, backward)

    zero = jnp.zeros((SUB, LANES), F32)
    ends = []
    signal_load.wait()
    for row in range(0, leak_ref.shape[0], 16):
        at = pl.ds(row, 16)
        rows_ref[at, :] = signal_ref[at, :].astype(F32) * scale
    for cut, load in zip(halves, leak_loads):
        load.wait()
        state = all_steps(groups, body, {g: (zero + 1.0, zero, zero) for g in cut})
        for g in cut:
            product, forward, backward = state[g]
            whole, forwards = scan_sublanes(product, forward, earlier_sublanes)
            turned, backwards = scan_sublanes(product, backward, later_sublanes)
            parts_ref[4 * g] = whole
            parts_ref[4 * g + 1] = forwards
            parts_ref[4 * g + 2] = turned
            parts_ref[4 * g + 3] = backwards
            ends.append((whole[SUB - 1 :], forwards[SUB - 1 :], backwards[:1]))
    product, forward, backward = ends[0][0], ends[0][1], ends[-1][2]
    for whole, forwards, _ in ends[1:]:
        product, forward = product * whole, forward * whole + forwards
    for whole, _, backwards in reversed(ends[:-1]):
        backward = backwards + whole * backward
    row = lax.broadcasted_iota(jnp.int32, (SUB, LANES), 0)
    packed = jnp.where(row == 0, product, jnp.where(row == 1, forward, backward))
    for copy in range(ends_ref.shape[0]):
        ends_ref[copy] = packed[: ends_ref.shape[1]]
    parts_ref[4 * len(groups)] = zero + here_ref[0].astype(F32)
    gain_load.wait()


def joined(pieces):
    while len(pieces) > 1:
        pieces = [
            (first[0] * second[0], first[1] * second[0] + second[1])
            for first, second in zip(pieces[::2], pieces[1::2])
        ]
    return pieces[0]


def states_kernel(
    order,
    all_ends_ref,
    parts_ref,
    keep_ref,
    push_ref,
    product_ref,
    forward_ref,
    gain_ref,
    states_ref,
    squares_ref,
):
    groups = groups_of(keep_ref.shape[0] * SUB)
    here = parts_ref[4 * len(groups), 0:1]
    devices = len(order)
    place = [order.index(d) for d in range(devices)]
    earlier, later = [], []
    for d in range(devices):
        product = all_ends_ref[place[d], 0:1]
        before, after = d < here, d > here
        earlier.append(
            (jnp.where(before, product, 1.0), jnp.where(before, all_ends_ref[place[d], 1:2], 0.0))
        )
        later.append(
            (jnp.where(after, product, 1.0), jnp.where(after, all_ends_ref[place[d], 2:3], 0.0))
        )
    forward = joined(earlier)[1]
    backward = joined(later[::-1])[1]

    entering_forward, entering_backward = [], [None] * len(groups)
    for g in range(len(groups)):
        whole, forwards = parts_ref[4 * g], parts_ref[4 * g + 1]
        entering_forward.append(
            earlier_sublanes(forwards, 1, 0.0) + earlier_sublanes(whole, 1, 1.0) * forward
        )
        forward = forwards[SUB - 1 :] + whole[SUB - 1 :] * forward
    for g in reversed(range(len(groups))):
        whole, backwards = parts_ref[4 * g + 2], parts_ref[4 * g + 3]
        entering_backward[g] = (
            later_sublanes(backwards, 1, 0.0) + later_sublanes(whole, 1, 1.0) * backward
        )
        backward = backwards[:1] + whole[:1] * backward

    gain = jnp.broadcast_to(gain_ref[...], (SUB, LANES))
    lane = lax.broadcasted_iota(jnp.int32, (SUB, LANES), 1)
    short = groups[0][2]

    def back(g, step, state):
        state, sums = state
        at = groups[g][1] + step
        state = state * keep_ref[at] + push_ref[at]
        both = (forward_ref[at] + product_ref[at] * entering_forward[g]) + state
        states_ref[at] = both * gain
        power = jnp.sum(both * both, axis=1, keepdims=True)
        sums = jnp.where(lane == step + (short if g >= 2 else 0), power, sums)
        return state, sums

    zero = jnp.zeros((SUB, LANES), F32)
    done = all_steps(groups, back, {g: (b, zero) for g, b in enumerate(entering_backward)}, reverse=True)
    for half in (0, 1):
        squares = jnp.where(lane < short, done[half][1], done[half + 2][1])
        squares_ref[pl.ds(half * SUB, SUB), :] = squares


def norm_kernel(channels, all_squares_ref, states_ref, out_hbm, rows_ref, out_ref, sent):
    groups = groups_of(rows_ref.shape[0])
    short = groups[0][2]
    power = jnp.sum(all_squares_ref[...], axis=0) / channels
    scale = lax.rsqrt(power + 1e-06)
    halves = (scale[:SUB], scale[SUB:])
    lanes = lax.broadcasted_iota(jnp.int32, (SUB, LANES), 1)
    stores = []
    for g, (first, at, length) in enumerate(groups):
        for step in range(length):
            lane = step + (short if g >= 2 else 0)
            factor = jnp.sum(jnp.where(lanes == lane, halves[g % 2], 0.0), axis=1, keepdims=True)
            rows_ref[rows_at(groups[g], step), :] = states_ref[at + step] * factor
        for row in range(first, first + length * SUB, 16):
            here = pl.ds(row, 16)
            out_ref[here, :] = rows_ref[here, :].astype(out_ref.dtype)
        if g % 2:
            rows = rows_of(groups, (g - 1, g))
            stores.append(pltpu.make_async_copy(out_ref.at[rows], out_hbm.at[rows], sent.at[g // 2]))
            stores[-1].start()
    for store in stores:
        store.wait()


def params():
    return pltpu.CompilerParams(vmem_limit_bytes=12 * 1024 * 1024)


def exchanged(x, axis, groups):
    return lax.all_to_all(x, axis, 0, 0, tiled=True, axis_index_groups=groups)


def per_device(leak_rate, signal_in, norm_gain):
    rows, channels = leak_rate.shape[1], leak_rate.shape[2]
    total_length = rows * lax.axis_size("seq")
    blocks = jax.ShapeDtypeStruct((rows // SUB, SUB, LANES), F32)
    here = lax.axis_index("seq").astype(jnp.int32).reshape(1)
    operands = (leak_rate[0], signal_in[0], norm_gain.reshape(1, channels))
    ends, *scanned = pl.pallas_call(
        functools.partial(summary_kernel, total_length),
        out_shape=(
            jax.ShapeDtypeStruct((lax.axis_size("seq"), 4, LANES), F32),
            jax.ShapeDtypeStruct((17, SUB, LANES), F32),
            blocks,
            blocks,
            blocks,
            blocks,
            jax.ShapeDtypeStruct((1, LANES), F32),
        ),
        in_specs=[SMEM] + [HBM] * 3,
        out_specs=(VMEM,) * 7,
        scratch_shapes=[
            pltpu.VMEM((rows, LANES), F32),
            pltpu.VMEM((rows, LANES), signal_in.dtype),
            pltpu.VMEM((rows, LANES), F32),
            pltpu.SemaphoreType.DMA((3,)),
            pltpu.SemaphoreType.DMA,
        ],
        compiler_params=params(),
        name="summary",
    )(here, *(pltpu.with_memory_space_constraint(x, pltpu.HBM) for x in operands))
    all_ends = exchanged(ends, "seq", [stretches()])
    states, squares = pl.pallas_call(
        functools.partial(states_kernel, stretches()),
        out_shape=(blocks, jax.ShapeDtypeStruct((2 * SUB, LANES), F32)),
        in_specs=[VMEM] * 7,
        out_specs=(VMEM,) * 2,
        compiler_params=params(),
        name="states",
    )(all_ends, *scanned)
    width = lax.axis_size("width")
    partners = [(member, member ^ 1) for member in range(width)]
    squares = squares + lax.ppermute(squares, "width", partners)
    squares = jnp.broadcast_to(squares[None], (width // CORES, *squares.shape))
    all_squares = exchanged(squares, "width", chips_of_each_core())
    mixed = pl.pallas_call(
        functools.partial(norm_kernel, channels * lax.axis_size("width")),
        out_shape=jax.ShapeDtypeStruct((rows, LANES), jnp.bfloat16),
        in_specs=[VMEM] * 2,
        out_specs=HBM,
        scratch_shapes=[
            pltpu.VMEM((rows, LANES), F32),
            pltpu.VMEM((rows, LANES), jnp.bfloat16),
            pltpu.SemaphoreType.DMA((2,)),
        ],
        compiler_params=params(),
        name="norm",
    )(all_squares, states)
    return mixed[None]


def solution(mesh):
    return jax.shard_map(
        per_device,
        mesh=mesh,
        in_specs=(P(None, "seq", "width"), P(None, "seq", "width"), P("width")),
        out_specs=P(None, "seq", "width"),
        check_vma=False,
    )
```

```python
import functools
import math

import jax
import jax.numpy as jnp
from jax import lax
from jax.experimental import pallas as pl
from jax.experimental.pallas import tpu as pltpu
from jax.sharding import PartitionSpec as P

LANES = 128
SUB = 8
F32 = jnp.float32
VMEM = pl.BlockSpec(memory_space=pltpu.VMEM)
SMEM = pl.BlockSpec(memory_space=pltpu.SMEM)
HBM = pl.BlockSpec(memory_space=pltpu.HBM)


FAR_STRETCH = 10
FAR_CHIP = 4
CORES = 2


def far_first(members, far):
    return [members[far % len(members)]] + [m for m in members if m != members[far % len(members)]]


def stretches():
    return far_first(list(range(lax.axis_size("seq"))), FAR_STRETCH)


def chips_of_each_core():
    size = lax.axis_size("width")
    return [far_first(list(range(core, size, CORES)), FAR_CHIP) for core in range(CORES)]


def groups_of(rows):
    steps = rows // SUB
    short = steps // 4 - 4
    assert rows % SUB == 0 and short % 8 == 4 and short + 68 <= LANES
    cuts, at = [], 0
    for length in (short, short, short + 8, short + 8):
        cuts.append((at * SUB, at, length))
        at += length
    assert at == steps
    return cuts


def rows_at(group, step):
    first, _, length = group
    return pl.ds(first + step, SUB, stride=length)


def earlier_sublanes(x, by, fill):
    row = lax.broadcasted_iota(jnp.int32, x.shape, 0)
    return jnp.where(row >= by, pltpu.roll(x, by, 0), fill)


def later_sublanes(x, by, fill):
    row = lax.broadcasted_iota(jnp.int32, x.shape, 0)
    return jnp.where(row < SUB - by, pltpu.roll(x, SUB - by, 0), fill)


def scan_sublanes(product, total, shifted):
    for by in (1, 2, 4):
        total = total + product * shifted(total, by, 0.0)
        product = product * shifted(product, by, 1.0)
    return product, total


def all_steps(groups, body, state, reverse=False):
    state = dict(state)
    longest = max(groups[g][2] for g in state)
    for step in reversed(range(longest)) if reverse else range(longest):
        for g in state:
            if step < groups[g][2]:
                state[g] = body(g, step, state[g])
    return state


def rows_of(groups, cut):
    return pl.ds(groups[cut[0]][0], sum(groups[g][2] for g in cut) * SUB)


def summary_kernel(
    total_length,
    here_ref,
    leak_hbm,
    signal_hbm,
    gain_hbm,
    ends_ref,
    parts_ref,
    keep_ref,
    push_ref,
    product_ref,
    forward_ref,
    gain_ref,
    leak_ref,
    signal_ref,
    rows_ref,
    arrived,
    gain_arrived,
):
    groups = groups_of(leak_ref.shape[0])
    scale = total_length ** (-0.5)
    exponent = -math.log2(math.e) / total_length
    halves = ((0, 1), (2, 3))
    signal_load = pltpu.make_async_copy(signal_hbm, signal_ref, arrived.at[0])
    signal_load.start()
    leak_loads = []
    for half, cut in enumerate(halves):
        at = rows_of(groups, cut)
        leak_loads.append(pltpu.make_async_copy(leak_hbm.at[at], leak_ref.at[at], arrived.at[1 + half]))
        leak_loads[-1].start()
    gain_load = pltpu.make_async_copy(gain_hbm, gain_ref, gain_arrived)
    gain_load.start()

    def body(g, step, state):
        product, forward, backward = state
        keep = jnp.exp2(leak_ref[rows_at(groups[g], step), :] * exponent)
        push = rows_ref[rows_at(groups[g], step), :]
        keep_ref[groups[g][1] + step] = keep
        push_ref[groups[g][1] + step] = push
        backward = backward + product * push
        product, forward = product * keep, forward * keep + push
        product_ref[groups[g][1] + step] = product
        forward_ref[groups[g][1] + step] = forward
        return (product, forward, backward)

    zero = jnp.zeros((SUB, LANES), F32)
    state = {}
    signal_load.wait()
    for row in range(0, leak_ref.shape[0], 16):
        at = pl.ds(row, 16)
        rows_ref[at, :] = signal_ref[at, :].astype(F32) * scale
    for cut, load in zip(halves, leak_loads):
        load.wait()
        state |= all_steps(groups, body, {g: (zero + 1.0, zero, zero) for g in cut})
    ends = []
    for g in range(len(groups)):
        product, forward, backward = state[g]
        whole, forwards = scan_sublanes(product, forward, earlier_sublanes)
        turned, backwards = scan_sublanes(product, backward, later_sublanes)
        parts_ref[4 * g] = whole
        parts_ref[4 * g + 1] = forwards
        parts_ref[4 * g + 2] = turned
        parts_ref[4 * g + 3] = backwards
        ends.append((whole[SUB - 1 :], forwards[SUB - 1 :], backwards[:1]))
    product, forward, backward = ends[0][0], ends[0][1], ends[-1][2]
    for whole, forwards, _ in ends[1:]:
        product, forward = product * whole, forward * whole + forwards
    for whole, _, backwards in reversed(ends[:-1]):
        backward = backwards + whole * backward
    row = lax.broadcasted_iota(jnp.int32, (SUB, LANES), 0)
    packed = jnp.where(row == 0, product, jnp.where(row == 1, forward, backward))
    for copy in range(ends_ref.shape[0]):
        ends_ref[copy] = packed[: ends_ref.shape[1]]
    parts_ref[4 * len(groups)] = zero + here_ref[0].astype(F32)
    gain_load.wait()


def joined(pieces):
    while len(pieces) > 1:
        pieces = [
            (first[0] * second[0], first[1] * second[0] + second[1])
            for first, second in zip(pieces[::2], pieces[1::2])
        ]
    return pieces[0]


def states_kernel(
    order,
    all_ends_ref,
    parts_ref,
    keep_ref,
    push_ref,
    product_ref,
    forward_ref,
    gain_ref,
    states_ref,
    squares_ref,
):
    groups = groups_of(keep_ref.shape[0] * SUB)
    here = parts_ref[4 * len(groups), 0:1]
    devices = len(order)
    place = [order.index(d) for d in range(devices)]
    earlier, later = [], []
    for d in range(devices):
        product = all_ends_ref[place[d], 0:1]
        before, after = d < here, d > here
        earlier.append(
            (jnp.where(before, product, 1.0), jnp.where(before, all_ends_ref[place[d], 1:2], 0.0))
        )
        later.append(
            (jnp.where(after, product, 1.0), jnp.where(after, all_ends_ref[place[d], 2:3], 0.0))
        )
    forward = joined(earlier)[1]
    backward = joined(later[::-1])[1]

    entering_forward, entering_backward = [], [None] * len(groups)
    for g in range(len(groups)):
        whole, forwards = parts_ref[4 * g], parts_ref[4 * g + 1]
        entering_forward.append(
            earlier_sublanes(forwards, 1, 0.0) + earlier_sublanes(whole, 1, 1.0) * forward
        )
        forward = forwards[SUB - 1 :] + whole[SUB - 1 :] * forward
    for g in reversed(range(len(groups))):
        whole, backwards = parts_ref[4 * g + 2], parts_ref[4 * g + 3]
        entering_backward[g] = (
            later_sublanes(backwards, 1, 0.0) + later_sublanes(whole, 1, 1.0) * backward
        )
        backward = backwards[:1] + whole[:1] * backward

    gain = jnp.broadcast_to(gain_ref[...], (SUB, LANES))
    lane = lax.broadcasted_iota(jnp.int32, (SUB, LANES), 1)
    short = groups[0][2]

    def back(g, step, state):
        state, sums = state
        at = groups[g][1] + step
        state = state * keep_ref[at] + push_ref[at]
        both = (forward_ref[at] + product_ref[at] * entering_forward[g]) + state
        states_ref[at] = both * gain
        power = jnp.sum(both * both, axis=1, keepdims=True)
        sums = jnp.where(lane == step + (short if g >= 2 else 0), power, sums)
        return state, sums

    zero = jnp.zeros((SUB, LANES), F32)
    done = all_steps(groups, back, {g: (b, zero) for g, b in enumerate(entering_backward)}, reverse=True)
    for half in (0, 1):
        squares = jnp.where(lane < short, done[half][1], done[half + 2][1])
        squares_ref[pl.ds(half * SUB, SUB), :] = squares


def norm_kernel(channels, all_squares_ref, states_ref, out_hbm, rows_ref, out_ref, sent):
    groups = groups_of(rows_ref.shape[0])
    short = groups[0][2]
    power = jnp.sum(all_squares_ref[...], axis=0) / channels
    scale = lax.rsqrt(power + 1e-06)
    halves = (scale[:SUB], scale[SUB:])
    lanes = lax.broadcasted_iota(jnp.int32, (SUB, LANES), 1)
    stores = []
    for g, (first, at, length) in enumerate(groups):
        for step in range(length):
            lane = step + (short if g >= 2 else 0)
            factor = jnp.sum(jnp.where(lanes == lane, halves[g % 2], 0.0), axis=1, keepdims=True)
            rows_ref[rows_at(groups[g], step), :] = states_ref[at + step] * factor
        for row in range(first, first + length * SUB, 16):
            here = pl.ds(row, 16)
            out_ref[here, :] = rows_ref[here, :].astype(out_ref.dtype)
        if g % 2:
            rows = rows_of(groups, (g - 1, g))
            stores.append(pltpu.make_async_copy(out_ref.at[rows], out_hbm.at[rows], sent.at[g // 2]))
            stores[-1].start()
    for store in stores:
        store.wait()


def params():
    return pltpu.CompilerParams(vmem_limit_bytes=12 * 1024 * 1024)


def exchanged(x, axis, groups):
    return lax.all_to_all(x, axis, 0, 0, tiled=True, axis_index_groups=groups)


def per_device(leak_rate, signal_in, norm_gain):
    rows, channels = leak_rate.shape[1], leak_rate.shape[2]
    total_length = rows * lax.axis_size("seq")
    blocks = jax.ShapeDtypeStruct((rows // SUB, SUB, LANES), F32)
    here = lax.axis_index("seq").astype(jnp.int32).reshape(1)
    operands = (leak_rate[0], signal_in[0], norm_gain.reshape(1, channels))
    ends, *scanned = pl.pallas_call(
        functools.partial(summary_kernel, total_length),
        out_shape=(
            jax.ShapeDtypeStruct((lax.axis_size("seq"), 4, LANES), F32),
            jax.ShapeDtypeStruct((17, SUB, LANES), F32),
            blocks,
            blocks,
            blocks,
            blocks,
            jax.ShapeDtypeStruct((1, LANES), F32),
        ),
        in_specs=[SMEM] + [HBM] * 3,
        out_specs=(VMEM,) * 7,
        scratch_shapes=[
            pltpu.VMEM((rows, LANES), F32),
            pltpu.VMEM((rows, LANES), signal_in.dtype),
            pltpu.VMEM((rows, LANES), F32),
            pltpu.SemaphoreType.DMA((3,)),
            pltpu.SemaphoreType.DMA,
        ],
        compiler_params=params(),
        name="summary",
    )(here, *(pltpu.with_memory_space_constraint(x, pltpu.HBM) for x in operands))
    all_ends = exchanged(ends, "seq", [stretches()])
    states, squares = pl.pallas_call(
        functools.partial(states_kernel, stretches()),
        out_shape=(blocks, jax.ShapeDtypeStruct((2 * SUB, LANES), F32)),
        in_specs=[VMEM] * 7,
        out_specs=(VMEM,) * 2,
        compiler_params=params(),
        name="states",
    )(all_ends, *scanned)
    width = lax.axis_size("width")
    partners = [(member, member ^ 1) for member in range(width)]
    squares = squares + lax.ppermute(squares, "width", partners)
    squares = jnp.broadcast_to(squares[None], (width // CORES, *squares.shape))
    all_squares = exchanged(squares, "width", chips_of_each_core())
    mixed = pl.pallas_call(
        functools.partial(norm_kernel, channels * lax.axis_size("width")),
        out_shape=jax.ShapeDtypeStruct((rows, LANES), jnp.bfloat16),
        in_specs=[VMEM] * 2,
        out_specs=HBM,
        scratch_shapes=[
            pltpu.VMEM((rows, LANES), F32),
            pltpu.VMEM((rows, LANES), jnp.bfloat16),
            pltpu.SemaphoreType.DMA((2,)),
        ],
        compiler_params=params(),
        name="norm",
    )(all_squares, states)
    return mixed[None]


def solution(mesh):
    return jax.shard_map(
        per_device,
        mesh=mesh,
        in_specs=(P(None, "seq", "width"), P(None, "seq", "width"), P("width")),
        out_specs=P(None, "seq", "width"),
        check_vma=False,
    )
```
